32 devices in a mesh: bank: 8 (over y, x, core), zero: 4 (over z).
Axes of the slice: x: 2, y: 2, z: 4, core: 2. Of those that a mesh axis runs over, the one named last changes fastest.
Arguments:
- master_down: float32 [64, 1024, 2048], P('bank', None, 'zero'), may hold values from -0.25 to 0.25
- router_weight: float32 [2048, 64], P('zero', 'bank'), may hold values from -0.125 to 0.125
- router_gain: float32 [2048], P('zero'), may hold values from 0.25 to 1.75
Outputs:
- final_down: bfloat16 [64, 1024, 2048], P('bank')
- scale_down: float32 [64, 1024], P('bank')
- serve_router: bfloat16 [2048, 64], replicated
The draws below stay inside these ranges and needn't reach their ends.
All inputs are finite; a program needn't handle non-finite values. Where the reference program divides by a largest or mean magnitude, that divisor is 1e-20 or more.
Results may differ from the reference program's by a relative error of at most 0.001.
Values may be sent and summed in bfloat16 or wider, within the bound.
A program may use at most 128 MiB of HBM per device.

```python
import jax
import jax.numpy as jnp

EXPERTS = 64
D_MODEL = 2048
D_EXPERT = 1024


def spiked(array, stream_key, source, target, shards_of, factor):
    def block_of(dim):
        return (jnp.arange(array.shape[dim]) // (array.shape[dim] // shards_of)).reshape((-1,) + (1,) * (array.ndim - 1 - dim))

    first = jax.random.permutation(stream_key, shards_of)[block_of(target)]
    second = (block_of(target) + shards_of // 2) % shards_of
    return jnp.where((block_of(source) == first) | (block_of(source) == second), factor * array, array)


def block_levels(rng, shape, pieces, least, high):
    loudness = 1.0
    for dim, blocks in pieces:
        steps = jax.random.uniform(jax.random.fold_in(jax.random.fold_in(rng, 6), dim), (blocks,), jnp.float32, least / len(pieces), high / len(pieces))
        loudness = loudness * jnp.repeat(jnp.exp(steps), shape[dim] // blocks).reshape((-1,) + (1,) * (len(shape) - 1 - dim))
    return loudness


def bell_draw(rng, extent, deviation, bound, pieces=(), dtype=jnp.bfloat16):
    drawn = deviation * jax.random.normal(rng, extent, jnp.float32)
    if pieces:
        drawn = drawn * block_levels(rng, extent, pieces, -0.22, 0.18)
    return jnp.clip(drawn, -bound, bound).astype(dtype)


def gaussian_with(rng, shape, scale, limit, pieces, heavy, dtype=jnp.bfloat16):
    entries = scale * jax.random.normal(rng, shape, jnp.float32)
    if pieces:
        entries = entries * block_levels(rng, shape, pieces, -0.22, 0.18)
    return jnp.clip(spiked(entries, jax.random.fold_in(rng, 3), *heavy), -limit, limit).astype(dtype)


def setup_inputs(seed: int = 0) -> dict:
    splits = jax.random.split(jax.random.key(seed), 4)
    master_down = gaussian_with(splits[0], (EXPERTS, D_EXPERT, D_MODEL), D_EXPERT ** -0.5, 0.25, ((0, 8), (2, 4)), (2, 1, 4, 2.0), jnp.float32)
    router_weight = bell_draw(splits[1], (D_MODEL, EXPERTS), D_MODEL ** -0.5, 0.125, ((0, 4), (1, 8)), jnp.float32)
    router_gain = jnp.clip(1.0 + 0.15 * jax.random.normal(splits[2], (D_MODEL,), jnp.float32), 0.25, 1.75)
    return dict(master_down=master_down, router_weight=router_weight, router_gain=router_gain)


def reference(master_down, router_weight, router_gain):
    scale_down = jnp.max(jnp.abs(master_down), axis=2)
    final_down = (master_down / jnp.expand_dims(scale_down, 2)).astype(jnp.bfloat16)
    serve_router = (router_weight * router_gain[:, None]).astype(jnp.bfloat16)
    return final_down, scale_down, serve_router
```

```python
import functools

import jax
import jax.numpy as jnp
from jax import lax
from jax.experimental import pallas as pl
from jax.experimental.pallas import tpu as pltpu
from jax.sharding import PartitionSpec as P

MESH = pl.DeviceIdType.MESH
LANES = 128
CHUNK = 512


def remote(src, dst, send, recv, axis, peer):
    return pltpu.make_async_remote_copy(
        src_ref=src, dst_ref=dst, send_sem=send, recv_sem=recv,
        device_id={axis: peer}, device_id_type=MESH,
    )


def gather_kernel(
    n, banks, m_ref, r_ref, t_ref, s_ref, g_out,
    x, nar, mx, g, in_sem, own_sem, ls, lr, rs, rr, ms, mr, zs, zr, bs, br,
):
    z, b = lax.axis_index("zero"), lax.axis_index("bank")
    rows, w = x.shape
    experts, groups = mx.shape[1:3]
    depth = groups * LANES
    chunks = rows // CHUNK
    per = depth // CHUNK

    def load(e):
        span = pl.ds(e * depth, depth)
        return pltpu.make_async_copy(m_ref.at[span], x.at[span], in_sem.at[e])

    def maxima(e):
        load(e).wait()

        def piece(i, _):
            base = e * depth + i * LANES
            top = jnp.abs(x[pl.ds(base, LANES), 0:LANES])
            for k in range(1, w // LANES):
                top = jnp.maximum(top, jnp.abs(x[pl.ds(base, LANES), k * LANES:(k + 1) * LANES]))
            mx[z, e, pl.ds(i, 1), :] = jnp.max(top.T, axis=0, keepdims=True)
            return 0

        lax.fori_loop(0, groups, piece, 0)

    def exchange(which, first, last):
        span = pl.ds(first, last - first)
        return [
            remote(mx.at[z, span], mx.at[z, span], ms.at[which, k - 1], mr.at[which, k - 1], "zero", lax.rem(z + k, n))
            for k in range(1, n)
        ]

    def narrow(c):
        def piece(j, _):
            row = c * CHUNK + j * LANES
            e, i = row // depth, (row % depth) // LANES
            s = mx[0, e, pl.ds(i, 1), :]
            for k in range(1, n):
                s = jnp.maximum(s, mx[k, e, pl.ds(i, 1), :])
            s_ref[e, pl.ds(i, 1), :] = s
            wide = jnp.broadcast_to(s, (LANES, LANES)).T
            for k in range(w // LANES):
                part = x[pl.ds(row, LANES), k * LANES:(k + 1) * LANES] / wide
                nar[pl.ds(row, LANES), k * LANES:(k + 1) * LANES] = part.astype(nar.dtype)
            return 0

        lax.fori_loop(0, CHUNK // LANES, piece, 0)

    def span_of(c):
        return pl.ds(pl.multiple_of(c * CHUNK, CHUNK), CHUNK)

    def place(c, o):
        return t_ref.at[span_of(c), pl.ds(pl.multiple_of(o * w, LANES), w)]

    def leftward(p, c):
        src = nar.at[span_of(c)] if p == 0 else place(c, z + p)
        return remote(src, place(c, z + p), ls.at[p, c], lr.at[p, c], "zero", z - 1)

    def rightward(p, c):
        src = nar.at[span_of(c)] if p == 0 else place(c, z - p)
        return remote(src, place(c, z - p), rs.at[p, c], rr.at[p, c], "zero", z + 1)

    def from_right(p, c):
        there = place(c, z + 1 + p)
        return remote(there, there, ls.at[p, c], lr.at[p, c], "zero", z + 1)

    def from_left(p, c):
        there = place(c, z - 1 - p)
        return remote(there, there, rs.at[p, c], rr.at[p, c], "zero", z - 1)

    def own(c):
        return pltpu.make_async_copy(nar.at[span_of(c)], place(c, z), own_sem.at[c])

    def send(c):
        @pl.when(z > 0)
        def _():
            leftward(0, c).start()

        @pl.when(z < n - 1)
        def _():
            rightward(0, c).start()

        own(c).start()

    def each(first, last, body):
        def step(c, _):
            body(c)
            return 0

        lax.fori_loop(first, last, step, 0)

    each(0, experts, lambda e: load(e).start())
    barrier = pltpu.get_barrier_semaphore()
    for k in range(1, n):
        pl.semaphore_signal(barrier, inc=1, device_id={"zero": lax.rem(z + k, n)}, device_id_type=MESH)
    for k in range(1, banks):
        pl.semaphore_signal(barrier, inc=1, device_id={"bank": lax.rem(b + k, banks)}, device_id_type=MESH)
    maxima(0)
    g[b, z] = r_ref[...]
    pl.semaphore_wait(barrier, n + banks - 2)

    early = exchange(0, 0, 1)
    for copy in early:
        copy.start()
    routes = [
        remote(g.at[b, z], g.at[b, z], zs.at[k - 1], zr.at[k - 1], "zero", lax.rem(z + k, n)) for k in range(1, n)
    ]
    for copy in routes:
        copy.start()
    if experts > 1:
        maxima(1)
    for copy in early:
        copy.wait_recv()
    each(0, per, narrow)
    each(0, per, send)
    late = []
    if experts > 1:
        each(2, experts, maxima)
        late = exchange(1, 1, experts)
        for copy in late:
            copy.start()
        for copy in late:
            copy.wait_recv()
        narrow(per)

        def follow(c):
            narrow(c)
            send(c - 1)

        each(per + 1, chunks, follow)
    for copy in routes:
        copy.wait_recv()
    if experts > 1:
        send(chunks - 1)
    spread = [
        remote(g.at[b], g.at[b], bs.at[k - 1], br.at[k - 1], "bank", lax.rem(b + k, banks)) for k in range(1, banks)
    ]
    for copy in spread:
        copy.start()

    for p in range(1, n):
        def relay(c):
            @pl.when(z + p <= n - 1)
            def _():
                from_right(p - 1, c).wait_recv()

            if p < n - 1:
                @pl.when((z > 0) & (z + p <= n - 1))
                def _():
                    leftward(p, c).start()

            @pl.when(z - p >= 0)
            def _():
                from_left(p - 1, c).wait_recv()

            if p < n - 1:
                @pl.when((z < n - 1) & (z - p >= 0))
                def _():
                    rightward(p, c).start()

        each(0, chunks, relay)

    for copy in spread:
        copy.wait_recv()
    g_out[...] = g[...]
    for copy in early + late + routes + spread:
        copy.wait_send()
    each(0, chunks, lambda c: own(c).wait())
    for p in range(n - 1):
        @pl.when((z > 0) & (z + p <= n - 1))
        def _():
            each(0, chunks, lambda c: leftward(p, c).wait_send())

        @pl.when((z < n - 1) & (z - p >= 0))
        def _():
            each(0, chunks, lambda c: rightward(p, c).wait_send())


def per_device(n, banks, master_down, router_weight, router_gain):
    experts, depth, w = master_down.shape
    part, few = router_weight.shape
    rows = experts * depth
    chunks = rows // CHUNK
    groups = depth // LANES
    part_router = (router_weight * router_gain[:, None]).astype(jnp.bfloat16).T
    dma = pltpu.SemaphoreType.DMA
    gathered, scale, routed = pl.pallas_call(
        functools.partial(gather_kernel, n, banks),
        out_shape=(
            jax.ShapeDtypeStruct((rows, n * w), jnp.bfloat16),
            jax.ShapeDtypeStruct((experts, groups, LANES), jnp.float32),
            jax.ShapeDtypeStruct((banks, n, few, part), jnp.bfloat16),
        ),
        in_specs=[pl.BlockSpec(memory_space=pl.ANY), pl.BlockSpec(memory_space=pltpu.VMEM)],
        out_specs=(
            pl.BlockSpec(memory_space=pl.ANY),
            pl.BlockSpec(memory_space=pltpu.VMEM),
            pl.BlockSpec(memory_space=pltpu.VMEM),
        ),
        scratch_shapes=[
            pltpu.VMEM((rows, w), jnp.float32),
            pltpu.VMEM((rows, w), jnp.bfloat16),
            pltpu.VMEM((n, experts, groups, LANES), jnp.float32),
            pltpu.VMEM((banks, n, few, part), jnp.bfloat16),
            dma((experts,)),
            dma((chunks,)),
            dma((n - 1, chunks)),
            dma((n - 1, chunks)),
            dma((n - 1, chunks)),
            dma((n - 1, chunks)),
            dma((2, n - 1)),
            dma((2, n - 1)),
            dma((n - 1,)),
            dma((n - 1,)),
            dma((banks - 1,)),
            dma((banks - 1,)),
        ],
        compiler_params=pltpu.CompilerParams(collective_id=0, has_side_effects=True),
        name="gather",
    )(master_down.reshape(rows, w), part_router)
    serve_router = routed.transpose(1, 3, 0, 2).reshape(n * part, banks * few)
    return (
        gathered.reshape(experts, depth, n * w),
        scale.reshape(experts, depth),
        serve_router,
    )


def solution(mesh):
    placed = (P("bank", None, "zero"), P("zero", "bank"), P("zero"))
    return jax.shard_map(
        functools.partial(per_device, mesh.shape["zero"], mesh.shape["bank"]),
        mesh=mesh,
        in_specs=placed,
        out_specs=(P("bank", None, None), P("bank", None), P()),
        check_vma=False,
    )
```

```python
import functools

import jax
import jax.numpy as jnp
from jax import lax
from jax.experimental import pallas as pl
from jax.experimental.pallas import tpu as pltpu
from jax.sharding import PartitionSpec as P

MESH = pl.DeviceIdType.MESH
LANES = 128
CHUNK = 512


def remote(src, dst, send, recv, axis, peer):
    return pltpu.make_async_remote_copy(
        src_ref=src, dst_ref=dst, send_sem=send, recv_sem=recv,
        device_id={axis: peer}, device_id_type=MESH,
    )


def gather_kernel(
    n, banks, ends, m_ref, r_ref, t_ref, u_ref, s_ref, g_out,
    x, nar, mx, g, in_sem, own_sem, ls, lr, rs, rr, ms, mr, zs, zr, bs, br,
):
    z, b = lax.axis_index("zero"), lax.axis_index("bank")
    rows, w = x.shape
    experts, groups = mx.shape[1:3]
    depth = groups * LANES
    chunks = rows // CHUNK
    per = depth // CHUNK
    body = chunks - ends

    def load(e):
        span = pl.ds(e * depth, depth)
        return pltpu.make_async_copy(m_ref.at[span], x.at[span], in_sem.at[e])

    def maxima(e):
        load(e).wait()

        def piece(i, _):
            base = e * depth + i * LANES
            top = jnp.abs(x[pl.ds(base, LANES), 0:LANES])
            for k in range(1, w // LANES):
                top = jnp.maximum(top, jnp.abs(x[pl.ds(base, LANES), k * LANES:(k + 1) * LANES]))
            mx[z, e, pl.ds(i, 1), :] = jnp.max(top.T, axis=0, keepdims=True)
            return 0

        lax.fori_loop(0, groups, piece, 0)

    def exchange(which, first, last):
        span = pl.ds(first, last - first)
        return [
            remote(mx.at[z, span], mx.at[z, span], ms.at[which, k - 1], mr.at[which, k - 1], "zero", lax.rem(z + k, n))
            for k in range(1, n)
        ]

    def narrow(c):
        def piece(j, _):
            row = c * CHUNK + j * LANES
            e, i = row // depth, (row % depth) // LANES
            s = mx[0, e, pl.ds(i, 1), :]
            for k in range(1, n):
                s = jnp.maximum(s, mx[k, e, pl.ds(i, 1), :])
            s_ref[e, pl.ds(i, 1), :] = s
            wide = jnp.broadcast_to(s, (LANES, LANES)).T
            for k in range(w // LANES):
                part = x[pl.ds(row, LANES), k * LANES:(k + 1) * LANES] / wide
                nar[pl.ds(row, LANES), k * LANES:(k + 1) * LANES] = part.astype(nar.dtype)
            return 0

        lax.fori_loop(0, CHUNK // LANES, piece, 0)

    def span_of(c):
        return pl.ds(pl.multiple_of(c * CHUNK, CHUNK), CHUNK)

    def place(c, o):
        return t_ref.at[span_of(c), pl.ds(pl.multiple_of(o * w, LANES), w)]

    def leftward(p, c):
        src = nar.at[span_of(c)] if p == 0 else place(c, z + p)
        return remote(src, place(c, z + p), ls.at[p, c], lr.at[p, c], "zero", z - 1)

    def rightward(p, c):
        src = nar.at[span_of(c)] if p == 0 else place(c, z - p)
        return remote(src, place(c, z - p), rs.at[p, c], rr.at[p, c], "zero", z + 1)

    def from_right(p, c):
        there = place(c, z + 1 + p)
        return remote(there, there, ls.at[p, c], lr.at[p, c], "zero", z + 1)

    def from_left(p, c):
        there = place(c, z - 1 - p)
        return remote(there, there, rs.at[p, c], rr.at[p, c], "zero", z - 1)

    def own(c):
        return pltpu.make_async_copy(nar.at[span_of(c)], place(c, z), own_sem.at[c])

    def slot(r, o):
        return u_ref.at[lax.rem(o - jnp.where(r <= 1, 1, 0) + n, n)]

    last = chunks - 1

    def last_leftward(p):
        src = nar.at[span_of(last)] if p == 0 else slot(z, z + p)
        return remote(src, slot(z - 1, z + p), ls.at[p, last], lr.at[p, last], "zero", z - 1)

    def last_rightward(p):
        src = nar.at[span_of(last)] if p == 0 else slot(z, z - p)
        return remote(src, slot(z + 1, z - p), rs.at[p, last], rr.at[p, last], "zero", z + 1)

    def last_from_right(p):
        there = slot(z, z + 1 + p)
        return remote(there, there, ls.at[p, last], lr.at[p, last], "zero", z + 1)

    def last_from_left(p):
        there = slot(z, z - 1 - p)
        return remote(there, there, rs.at[p, last], rr.at[p, last], "zero", z - 1)

    def last_own():
        return pltpu.make_async_copy(nar.at[span_of(last)], slot(z, z), own_sem.at[last])

    inner = (z > 0) & (z < n - 1)
    goes_left, goes_right = z > 1, z < n - 2

    def send_last():
        @pl.when(goes_left)
        def _():
            last_leftward(0).start()

        @pl.when(goes_right)
        def _():
            last_rightward(0).start()

        last_own().start()

    def send(c):
        @pl.when(z > 0)
        def _():
            leftward(0, c).start()

        @pl.when(z < n - 1)
        def _():
            rightward(0, c).start()

        own(c).start()

    def each(first, last, body):
        def step(c, _):
            body(c)
            return 0

        lax.fori_loop(first, last, step, 0)

    each(0, experts, lambda e: load(e).start())
    barrier = pltpu.get_barrier_semaphore()
    for k in range(1, n):
        pl.semaphore_signal(barrier, inc=1, device_id={"zero": lax.rem(z + k, n)}, device_id_type=MESH)
    for k in range(1, banks):
        pl.semaphore_signal(barrier, inc=1, device_id={"bank": lax.rem(b + k, banks)}, device_id_type=MESH)
    maxima(0)
    g[b, z] = r_ref[...]
    pl.semaphore_wait(barrier, n + banks - 2)

    early = exchange(0, 0, 1)
    for copy in early:
        copy.start()
    routes = [
        remote(g.at[b, z], g.at[b, z], zs.at[k - 1], zr.at[k - 1], "zero", lax.rem(z + k, n)) for k in range(1, n)
    ]
    for copy in routes:
        copy.start()
    late = []
    if experts > 1:
        each(1, experts, maxima)
        late = exchange(1, 1, experts)
        for copy in late:
            copy.start()
    for copy in early:
        copy.wait_recv()
    narrow(0)

    def follow(c):
        narrow(c)
        send(c - 1)

    each(1, per, follow)
    for copy in late:
        copy.wait_recv()
    each(per, chunks, follow)
    for copy in routes:
        copy.wait_recv()
    if ends:
        send_last()
    else:
        send(last)
    spread = [
        remote(g.at[b], g.at[b], bs.at[k - 1], br.at[k - 1], "bank", lax.rem(b + k, banks)) for k in range(1, banks)
    ]
    for copy in spread:
        copy.start()

    for p in range(1, n):
        def relay(c):
            @pl.when(z + p <= n - 1)
            def _():
                from_right(p - 1, c).wait_recv()

            if p < n - 1:
                @pl.when((z > 0) & (z + p <= n - 1))
                def _():
                    leftward(p, c).start()

            @pl.when(z - p >= 0)
            def _():
                from_left(p - 1, c).wait_recv()

            if p < n - 1:
                @pl.when((z < n - 1) & (z - p >= 0))
                def _():
                    rightward(p, c).start()

        each(0, body, relay)
        if ends:
            @pl.when(inner & (z + p <= n - 1))
            def _():
                last_from_right(p - 1).wait_recv()

            if p < n - 1:
                @pl.when(goes_left & (z < n - 1) & (z + p <= n - 1))
                def _():
                    last_leftward(p).start()

            @pl.when(inner & (z - p >= 0))
            def _():
                last_from_left(p - 1).wait_recv()

            if p < n - 1:
                @pl.when(goes_right & (z > 0) & (z - p >= 0))
                def _():
                    last_rightward(p).start()

    for copy in spread:
        copy.wait_recv()
    g_out[...] = g[...]
    for copy in early + late + routes + spread:
        copy.wait_send()
    each(0, body, lambda c: own(c).wait())
    if ends:
        last_own().wait()
    for p in range(n - 1):
        @pl.when((z > 0) & (z + p <= n - 1))
        def _():
            each(0, body, lambda c: leftward(p, c).wait_send())

        @pl.when((z < n - 1) & (z - p >= 0))
        def _():
            each(0, body, lambda c: rightward(p, c).wait_send())

        if ends:
            @pl.when(goes_left & (z + p <= n - 1))
            def _():
                last_leftward(p).wait_send()

            @pl.when(goes_right & (z - p >= 0))
            def _():
                last_rightward(p).wait_send()


def copy_kernel(t_ref, o_ref):
    o_ref[...] = t_ref[...]


def last_kernel(slots, info, a_ref, u_ref, _, o_ref):
    take = (info[1] == 1) & (pl.program_id(0) < slots)

    @pl.when(take)
    def _():
        o_ref[...] = a_ref[0]

    @pl.when(jnp.logical_not(take))
    def _():
        o_ref[...] = u_ref[0]


def finish(n, body, rows, w, gathered, held):
    whole = jax.ShapeDtypeStruct((rows, n * w), jnp.bfloat16)
    arrived = lax.ppermute(held[:n - 1], "zero", ((1, 0), (n - 2, n - 1)))
    most = pl.pallas_call(
        copy_kernel,
        grid=(body,),
        out_shape=whole,
        in_specs=[pl.BlockSpec((CHUNK, n * w), lambda i: (i, 0))],
        out_specs=pl.BlockSpec((CHUNK, n * w), lambda i: (i, 0)),
        cost_estimate=pl.CostEstimate(flops=0, bytes_accessed=4 * body * CHUNK * n * w, transcendentals=0),
        name="most",
    )(gathered)
    z = lax.axis_index("zero")
    info = jnp.stack([jnp.where(z <= 1, 1, 0), jnp.where((z == 0) | (z == n - 1), 1, 0)]).astype(jnp.int32)
    return pl.pallas_call(
        functools.partial(last_kernel, n - 1),
        grid_spec=pltpu.PrefetchScalarGridSpec(
            num_scalar_prefetch=1,
            grid=(n,),
            in_specs=[
                pl.BlockSpec((1, CHUNK, w), lambda k, info: (jnp.minimum(k, n - 2), 0, 0)),
                pl.BlockSpec((1, CHUNK, w), lambda k, info: (k, 0, 0)),
                pl.BlockSpec(memory_space=pl.ANY),
            ],
            out_specs=pl.BlockSpec((CHUNK, w), lambda k, info: (body, lax.rem(k + info[0], n))),
        ),
        out_shape=whole,
        input_output_aliases={3: 0},
        name="last",
    )(info, arrived, held, most)


def per_device(n, banks, master_down, router_weight, router_gain):
    experts, depth, w = master_down.shape
    part, few = router_weight.shape
    rows = experts * depth
    chunks = rows // CHUNK
    groups = depth // LANES
    ends = 1 if n > 3 else 0
    body = chunks - ends
    part_router = (router_weight * router_gain[:, None]).astype(jnp.bfloat16).T
    dma = pltpu.SemaphoreType.DMA
    gathered, held, scale, routed = pl.pallas_call(
        functools.partial(gather_kernel, n, banks, ends),
        out_shape=(
            jax.ShapeDtypeStruct((body * CHUNK, n * w), jnp.bfloat16),
            jax.ShapeDtypeStruct((n, CHUNK, w), jnp.bfloat16),
            jax.ShapeDtypeStruct((experts, groups, LANES), jnp.float32),
            jax.ShapeDtypeStruct((banks, n, few, part), jnp.bfloat16),
        ),
        in_specs=[pl.BlockSpec(memory_space=pl.ANY), pl.BlockSpec(memory_space=pltpu.VMEM)],
        out_specs=(
            pl.BlockSpec(memory_space=pl.ANY),
            pl.BlockSpec(memory_space=pl.ANY),
            pl.BlockSpec(memory_space=pltpu.VMEM),
            pl.BlockSpec(memory_space=pltpu.VMEM),
        ),
        scratch_shapes=[
            pltpu.VMEM((rows, w), jnp.float32),
            pltpu.VMEM((rows, w), jnp.bfloat16),
            pltpu.VMEM((n, experts, groups, LANES), jnp.float32),
            pltpu.VMEM((banks, n, few, part), jnp.bfloat16),
            dma((experts,)),
            dma((chunks,)),
            dma((n - 1, chunks)),
            dma((n - 1, chunks)),
            dma((n - 1, chunks)),
            dma((n - 1, chunks)),
            dma((2, n - 1)),
            dma((2, n - 1)),
            dma((n - 1,)),
            dma((n - 1,)),
            dma((banks - 1,)),
            dma((banks - 1,)),
        ],
        compiler_params=pltpu.CompilerParams(collective_id=0, has_side_effects=True),
        name="gather",
    )(master_down.reshape(rows, w), part_router)
    if ends:
        gathered = finish(n, body, rows, w, gathered, held)
    serve_router = routed.transpose(1, 3, 0, 2).reshape(n * part, banks * few)
    return (
        gathered.reshape(experts, depth, n * w),
        scale.reshape(experts, depth),
        serve_router,
    )


def solution(mesh):
    placed = (P("bank", None, "zero"), P("zero", "bank"), P("zero"))
    return jax.shard_map(
        functools.partial(per_device, mesh.shape["zero"], mesh.shape["bank"]),
        mesh=mesh,
        in_specs=placed,
        out_specs=(P("bank", None, None), P("bank", None), P()),
        check_vma=False,
    )
```
